32 devices in a mesh: dp: 2 (over core), expert: 16 (over z, y, x).
Axes of the slice: x: 2, y: 2, z: 4, core: 2. Of those that a mesh axis runs over, the one named last changes fastest.
Arguments:
- tokens: bfloat16 [8192, 1024], P(('dp', 'expert')), may hold values from -6 to 6
- ln_gain: float32 [1024], replicated, may hold values from 0.5 to 1.5
- router_weight: bfloat16 [1024, 16], replicated
- routes_expert: int32 [8192], P(('dp', 'expert')), may hold values from 0 to 15, as said below
- route_slot: int32 [8192], P(('dp', 'expert')), may hold values from -1 to 3, as said below
- w_in: bfloat16 [16, 1024, 4096], P('expert', None, 'dp'), may hold values from -0.1875 to 0.1875
- w_out: bfloat16 [16, 4096, 1024], P('expert', 'dp'), may hold values from -0.09375 to 0.09375
Outputs:
- mixed: bfloat16 [8192, 1024], P(('dp', 'expert'))
- expert_update: bfloat16 [8192, 1024], P(('dp', 'expert'))
The draws below stay inside these ranges and needn't reach their ends.
Inputs may be any that keep to these rules, and one draw needn't show every extreme that they name: `routes_expert`: every expert is chosen by some token. route_slot[t] is the number of earlier tokens of the same device (the same aligned block of 256 tokens) routed to the same expert, or -1 where that number is 4 or more; the value 4 - 1 occurs in every draw.
All inputs are finite; a program needn't handle non-finite values.
Results may differ from the reference program's by a relative error of at most 0.0058.
Values may be sent and summed in bfloat16 or wider, within the bound.
No kernel may reach another device: no remote copies, remote signals or barrier semaphores. Data moves between devices by JAX's collectives and lax.ppermute only.
A program may use at most 64 MiB of HBM per device.

```python
import jax
import jax.numpy as jnp
from jax import lax

D = 1024
HID = 4096
CAP = 4
TOK_DEV = 256
EXPERTS = 16
TOKENS = 8192


def route_pair(key):
    key = jax.random.fold_in(key, 11)
    first, second = jax.random.split(key)
    hot_list = jax.random.permutation(first, EXPERTS)[:8].astype(jnp.int32)
    drawn = jax.random.randint(second, (TOKENS,), 0, 4 * EXPERTS).astype(jnp.int32)
    result = drawn % EXPERTS
    hot_pick = hot_list[(drawn - 3 * EXPERTS) % 8]
    chosen = jnp.where(drawn < 3 * EXPERTS, result, hot_pick).astype(jnp.int32)
    blocks = chosen.reshape(TOKENS // TOK_DEV, TOK_DEV)
    onehot = (blocks[:, :, None] == jnp.arange(EXPERTS, dtype=jnp.int32)[None, None, :]).astype(jnp.int32)
    rank = jnp.sum(jnp.cumsum(onehot, axis=1) * onehot, axis=2) - 1
    slots = jnp.where(rank < CAP, rank, -1).astype(jnp.int32).reshape(TOKENS)
    return (chosen, slots)


def draw_routes_expert(key, part):
    return route_pair(key)[0]


def draw_route_slot(key, part):
    return route_pair(key)[1]


def draw_router_weight(key, part):
    key = jax.random.fold_in(key, 23)
    first, second = jax.random.split(key, 2)
    column_scale = jnp.exp(jax.random.uniform(first, (EXPERTS,), jnp.float32, jnp.log(1.0), jnp.log(12.0)))
    entries = jax.random.normal(second, (D, EXPERTS), jnp.float32)
    return (entries * column_scale[None, :] / jnp.sqrt(1.0 * D)).astype(jnp.bfloat16)


def block_scale(rng, extent, cuts, low, top_value):
    def one(dim, shards_of):
        heights = jax.random.uniform(jax.random.fold_in(jax.random.fold_in(rng, 6), dim), (shards_of,), jnp.float32, low / len(cuts), top_value / len(cuts))
        return jnp.repeat(jnp.exp(heights), extent[dim] // shards_of).reshape((-1,) + (1,) * (len(extent) - dim - 1))

    level = one(*cuts[0])
    for cut in cuts[1:]:
        level = level * one(*cut)
    return level


def scatter_about(stream_key, extent, deviation, most, shards=(), kind=jnp.bfloat16):
    level = block_scale(stream_key, extent, shards, -0.22, 0.18) if shards else 1.0
    array = jax.random.normal(stream_key, extent, jnp.float32) * deviation * level
    return jnp.minimum(jnp.maximum(array, -most), most).astype(kind)


def setup_inputs(seed: int = 0) -> dict:
    seeds = jax.random.split(jax.random.key(seed), 8)
    return {
        "tokens": scatter_about(seeds[0], (TOKENS, D), 1.0, 6.0, ((0, 32),)),
        "ln_gain": jnp.clip(1.0 + 0.1 * jax.random.normal(seeds[1], (D,), jnp.float32), 0.5, 1.5),
        "router_weight": draw_router_weight(jax.random.fold_in(seeds[7], 71), 0),
        "routes_expert": draw_routes_expert(jax.random.fold_in(seeds[7], 71), 0),
        "route_slot": draw_route_slot(jax.random.fold_in(seeds[7], 71), 0),
        "w_in": scatter_about(seeds[5], (EXPERTS, D, HID), D ** -0.5, 0.1875, ((0, 16), (2, 2))),
        "w_out": scatter_about(seeds[6], (EXPERTS, HID, D), HID ** -0.5, 0.09375, ((0, 16), (1, 2))),
    }


def reference(tokens, ln_gain, router_weight, routes_expert, route_slot, w_in, w_out):
    values = tokens.astype(jnp.float32)
    mean = lax.optimization_barrier(jnp.mean(values, axis=1, keepdims=True))
    var = lax.optimization_barrier(jnp.mean((values - mean) ** 2, axis=1, keepdims=True))
    normed = ((values - mean) * lax.rsqrt(var + 1e-06) * ln_gain[None, :]).astype(jnp.bfloat16)
    logits = jnp.dot(normed, router_weight, preferred_element_type=jnp.float32)
    probs = jax.nn.softmax(logits, axis=1)
    gate = jnp.take_along_axis(probs, routes_expert[:, None].astype(jnp.int32), axis=1)[:, 0]
    sources = TOKENS // TOK_DEV
    source = (jnp.arange(TOKENS, dtype=jnp.int32) // TOK_DEV).astype(jnp.int32)
    kept = route_slot >= 0
    total_rows = EXPERTS * sources * CAP
    flat = jnp.where(kept, (routes_expert * sources + source) * CAP + route_slot, total_rows).astype(jnp.int32)
    width = tokens.shape[1]
    buffer = jnp.zeros((total_rows, width), jnp.bfloat16).at[flat].set(normed, mode='drop')
    buffer = buffer.reshape(EXPERTS, sources * CAP, width)

    def serve_expert(operands):
        rows, weight_in, weight_out = operands
        hidden = jax.nn.gelu(jnp.dot(rows, weight_in, preferred_element_type=jnp.float32), approximate=True).astype(jnp.bfloat16)
        return jnp.dot(hidden, weight_out, preferred_element_type=jnp.float32).astype(jnp.bfloat16)
    outputs = lax.map(serve_expert, (buffer, w_in, w_out)).reshape(total_rows, width)
    back = outputs[jnp.minimum(flat, total_rows - 1)]
    update = jnp.where(kept[:, None], back, jnp.zeros_like(back))
    mixed = (values + gate[:, None] * update.astype(jnp.float32)).astype(jnp.bfloat16)
    return (mixed, update)
```

```python
import functools

import jax
import jax.numpy as jnp
from jax import lax
from jax.experimental import pallas as pl
from jax.experimental.pallas import tpu as pltpu
from jax.sharding import PartitionSpec as P

CAP = 4
EPS = 1e-06
MIB = 1024 * 1024


def slot_of(expert_ref, slot_ref):
    expert = expert_ref[...]
    slot = slot_ref[...]
    return jnp.where(slot >= 0, expert * CAP + slot, -1)


def dispatch_body(tokens_ref, gain_ref, expert_ref, slot_ref, out_ref):
    slots, count = out_ref.shape[0], tokens_ref.shape[0]
    flat = slot_of(expert_ref, slot_ref)
    rows = lax.broadcasted_iota(jnp.int32, (slots, count), 0)
    select = jnp.where(rows == flat, 1.0, 0.0).astype(jnp.bfloat16)
    values = jnp.dot(select, tokens_ref[...], preferred_element_type=jnp.float32)
    mean = jnp.mean(values, axis=1, keepdims=True)
    centred = values - mean
    var = jnp.mean(centred * centred, axis=1, keepdims=True)
    normed = centred * lax.rsqrt(var + EPS) * gain_ref[...]
    out_ref[...] = normed.astype(jnp.bfloat16)


def gate_body(normed_ref, router_ref, expert_ref, slot_ref, pick_ref, gate_ref):
    count, slots = pick_ref.shape
    logits = lax.dot_general(
        router_ref[...],
        normed_ref[...],
        (((1,), (1,)), ((), ())),
        preferred_element_type=jnp.float32,
    )
    top = jnp.max(logits, axis=0, keepdims=True)
    exps = jnp.exp(logits - top)
    probs = exps / jnp.sum(exps, axis=0, keepdims=True)
    owner = lax.broadcasted_iota(jnp.int32, probs.shape, 1) // CAP
    expert = lax.broadcasted_iota(jnp.int32, probs.shape, 0)
    slot_gate = jnp.sum(jnp.where(owner == expert, probs, 0.0), axis=0, keepdims=True)
    flat = slot_of(expert_ref, slot_ref)
    column = jnp.transpose(jnp.broadcast_to(flat, (128, count)))[:, :1]
    picked = column == lax.broadcasted_iota(jnp.int32, (count, slots), 1)
    pick_ref[...] = jnp.where(picked, 1.0, 0.0).astype(jnp.bfloat16)
    gate = jnp.sum(jnp.where(picked, slot_gate, 0.0), axis=1, keepdims=True)
    gate_ref[...] = jnp.broadcast_to(gate, gate_ref.shape)


def gelu(v):
    inner = 0.7978845608028654 * (v + 0.044715 * (v * v * v))
    return 0.5 * v * (1.0 + jnp.tanh(inner))


def expert_body(own_ref, other_ref, w_in_ref, w_out_ref, keep_ref, send_ref, *, chunk):
    own = own_ref.shape[0]
    rows = jnp.concatenate([own_ref[...], other_ref[...]], axis=0)
    total = None
    for start in range(0, w_in_ref.shape[1], chunk):
        hidden = jnp.dot(
            rows, w_in_ref[:, start : start + chunk], preferred_element_type=jnp.float32
        )
        hidden = gelu(hidden).astype(jnp.bfloat16)
        part = jnp.dot(
            hidden, w_out_ref[start : start + chunk, :], preferred_element_type=jnp.float32
        )
        total = part if total is None else total + part
    keep_ref[...] = total[:own]
    send_ref[...] = total[own:]


def combine_body(tokens_ref, pick_ref, gate_ref, back_ref, mixed_ref, update_ref):
    update = jnp.dot(pick_ref[...], back_ref[...], preferred_element_type=jnp.float32)
    update_ref[...] = update.astype(jnp.bfloat16)
    mixed = tokens_ref[...].astype(jnp.float32) + gate_ref[:, :1] * update
    mixed_ref[...] = mixed.astype(jnp.bfloat16)


def params(limit):
    return pltpu.CompilerParams(vmem_limit_bytes=limit * MIB)


def per_device(tokens, ln_gain, router_weight, routes_expert, route_slot, w_in, w_out):
    count, width = tokens.shape
    experts = router_weight.shape[1]
    slots = experts * CAP
    swap = [(0, 1), (1, 0)]
    expert_row = routes_expert.reshape(1, count)
    slot_row = route_slot.reshape(1, count)
    outgoing = pl.pallas_call(
        dispatch_body,
        out_shape=jax.ShapeDtypeStruct((slots, width), jnp.bfloat16),
        compiler_params=params(8),
        name="dispatch",
    )(tokens, ln_gain.reshape(1, width), expert_row, slot_row)
    own = lax.all_to_all(
        outgoing.reshape(experts, CAP, width), "expert", split_axis=0, concat_axis=0, tiled=True
    ).reshape(slots, width)
    other = lax.ppermute(own, "dp", swap)
    pick, gate = pl.pallas_call(
        gate_body,
        out_shape=(
            jax.ShapeDtypeStruct((count, slots), jnp.bfloat16),
            jax.ShapeDtypeStruct((count, 128), jnp.float32),
        ),
        compiler_params=params(8),
        name="gate",
    )(outgoing, router_weight.T, expert_row, slot_row)
    keep, send = pl.pallas_call(
        functools.partial(expert_body, chunk=512),
        out_shape=(
            jax.ShapeDtypeStruct((slots, width), jnp.float32),
            jax.ShapeDtypeStruct((slots, width), jnp.float32),
        ),
        compiler_params=params(30),
        name="experts",
    )(own, other, w_in[0], w_out[0])
    summed = (keep + lax.ppermute(send, "dp", swap)).astype(jnp.bfloat16)
    back = lax.all_to_all(
        summed.reshape(experts, CAP, width), "expert", split_axis=0, concat_axis=0, tiled=True
    ).reshape(slots, width)
    block = count // 2
    mixed, update = pl.pallas_call(
        combine_body,
        grid=(count // block,),
        in_specs=[
            pl.BlockSpec((block, width), lambda i: (i, 0)),
            pl.BlockSpec((block, slots), lambda i: (i, 0)),
            pl.BlockSpec((block, 128), lambda i: (i, 0)),
            pl.BlockSpec((slots, width), lambda i: (0, 0)),
        ],
        out_specs=[
            pl.BlockSpec((block, width), lambda i: (i, 0)),
            pl.BlockSpec((block, width), lambda i: (i, 0)),
        ],
        out_shape=(
            jax.ShapeDtypeStruct((count, width), jnp.bfloat16),
            jax.ShapeDtypeStruct((count, width), jnp.bfloat16),
        ),
        compiler_params=params(12),
        name="combine",
    )(tokens, pick, gate, back)
    return (mixed, update)


def solution(mesh):
    in_specs = (
        P(("dp", "expert"), None),
        P(),
        P(),
        P(("dp", "expert")),
        P(("dp", "expert")),
        P("expert", None, "dp"),
        P("expert", "dp", None),
    )
    out_specs = (P(("dp", "expert"), None), P(("dp", "expert"), None))
    return jax.shard_map(
        per_device, mesh=mesh, in_specs=in_specs, out_specs=out_specs, check_vma=False
    )
```

```python
import functools

import jax
import jax.numpy as jnp
from jax import lax
from jax.experimental import pallas as pl
from jax.experimental.pallas import tpu as pltpu
from jax.sharding import PartitionSpec as P

CAP = 4
EPS = 1e-06
MIB = 1024 * 1024


def rotation(count):
    return (5 * count) // 8


def slot_of(expert, slot, experts):
    place = (expert + (experts - rotation(experts))) % experts
    return jnp.where(slot >= 0, place * CAP + slot, -1)


def open_body(out_ref):
    out_ref[...] = jnp.zeros(out_ref.shape, out_ref.dtype)


def select_body(opened_ref, tokens_ref, expert_ref, slot_ref, out_ref):
    del opened_ref
    slots, count = out_ref.shape[0], tokens_ref.shape[0]
    flat = slot_of(expert_ref[...], slot_ref[...], slots // CAP)
    rows = lax.broadcasted_iota(jnp.int32, (slots, count), 0)
    select = jnp.where(rows == flat, 1.0, 0.0).astype(jnp.bfloat16)
    out_ref[...] = jnp.dot(select, tokens_ref[...], preferred_element_type=jnp.float32)


def norm_body(values_ref, gain_ref, out_ref):
    values = values_ref[...]
    mean = jnp.mean(values, axis=1, keepdims=True)
    centred = values - mean
    var = jnp.mean(centred * centred, axis=1, keepdims=True)
    normed = centred * lax.rsqrt(var + EPS) * gain_ref[...]
    out_ref[...] = normed.reshape(out_ref.shape).astype(jnp.bfloat16)


def gate_body(normed_ref, router_ref, expert_ref, slot_ref, after_ref, pick_ref, gate_ref):
    del after_ref
    count, slots = pick_ref.shape
    experts = router_ref.shape[0]
    logits = lax.dot_general(
        router_ref[...],
        normed_ref[...].reshape(slots, normed_ref.shape[2]),
        (((1,), (1,)), ((), ())),
        preferred_element_type=jnp.float32,
    )
    top = jnp.max(logits, axis=0, keepdims=True)
    exps = jnp.exp(logits - top)
    probs = exps / jnp.sum(exps, axis=0, keepdims=True)
    place = lax.broadcasted_iota(jnp.int32, probs.shape, 1) // CAP
    owner = (place + rotation(experts)) % experts
    expert = lax.broadcasted_iota(jnp.int32, probs.shape, 0)
    slot_gate = jnp.sum(jnp.where(owner == expert, probs, 0.0), axis=0, keepdims=True)
    flat = slot_of(expert_ref[...], slot_ref[...], experts)
    column = jnp.transpose(jnp.broadcast_to(flat, (128, count)))[:, :1]
    picked = column == lax.broadcasted_iota(jnp.int32, (count, slots), 1)
    pick_ref[...] = jnp.where(picked, 1.0, 0.0).astype(jnp.bfloat16)
    gate = jnp.sum(jnp.where(picked, slot_gate, 0.0), axis=1, keepdims=True)
    gate_ref[...] = jnp.broadcast_to(gate, gate_ref.shape)


def gelu(v):
    inner = 0.7978845608028654 * (v + 0.044715 * (v * v * v))
    return 0.5 * v * (1.0 + jnp.tanh(inner))


def expert_body(rows_ref, w_in_ref, w_out_ref, out_ref, *, chunk):
    rows = rows_ref[...].reshape(out_ref.shape)
    total = None
    for start in range(0, w_in_ref.shape[1], chunk):
        hidden = jnp.dot(
            rows, w_in_ref[:, start : start + chunk], preferred_element_type=jnp.float32
        )
        hidden = gelu(hidden).astype(jnp.bfloat16)
        part = jnp.dot(
            hidden, w_out_ref[start : start + chunk, :], preferred_element_type=jnp.float32
        )
        total = part if total is None else total + part
    out_ref[...] = total


def join_body(keep_ref, other_ref, after_ref, out_ref):
    del after_ref
    total = keep_ref[...] + other_ref[...]
    out_ref[...] = total.reshape(out_ref.shape).astype(jnp.bfloat16)


def combine_body(tokens_ref, pick_ref, gate_ref, back_ref, mixed_ref, update_ref):
    back = back_ref[...].reshape(pick_ref.shape[1], back_ref.shape[2])
    update = jnp.dot(pick_ref[...], back, preferred_element_type=jnp.float32)
    update_ref[...] = update.astype(jnp.bfloat16)
    mixed = tokens_ref[...].astype(jnp.float32) + gate_ref[:, :1] * update
    mixed_ref[...] = mixed.astype(jnp.bfloat16)


def params(limit):
    return pltpu.CompilerParams(vmem_limit_bytes=limit * MIB)


def exchange(blocks):
    count = blocks.shape[0]
    group = [(i + rotation(count)) % count for i in range(count)]
    return lax.all_to_all(
        blocks, "expert", split_axis=0, concat_axis=0, tiled=True, axis_index_groups=[group]
    )


def per_device(tokens, ln_gain, router_weight, routes_expert, route_slot, w_in, w_out):
    count, width = tokens.shape
    experts = router_weight.shape[1]
    slots = experts * CAP
    swap = [(0, 1), (1, 0)]
    anywhere = pl.BlockSpec(memory_space=pl.ANY)
    whole = pl.BlockSpec(memory_space=pltpu.VMEM)
    expert_row = routes_expert.reshape(1, count)
    slot_row = route_slot.reshape(1, count)
    long = pl.CostEstimate(flops=20 * 10**9, bytes_accessed=32 * MIB, transcendentals=0)
    opened = pl.pallas_call(
        open_body,
        out_shape=jax.ShapeDtypeStruct((8, 128), jnp.float32),
        compiler_params=params(8),
        cost_estimate=long,
        name="open",
    )()
    values = pl.pallas_call(
        select_body,
        in_specs=[anywhere] + [whole] * 3,
        out_shape=jax.ShapeDtypeStruct((slots, width), jnp.float32),
        compiler_params=params(8),
        name="select",
    )(opened, tokens, expert_row, slot_row)
    outgoing = pl.pallas_call(
        norm_body,
        out_shape=jax.ShapeDtypeStruct((experts, CAP, width), jnp.bfloat16),
        compiler_params=params(8),
        cost_estimate=long,
        name="norm",
    )(values, ln_gain.reshape(1, width))
    own = exchange(outgoing)
    other = lax.ppermute(own, "dp", swap)
    serve = pl.pallas_call(
        functools.partial(expert_body, chunk=512),
        out_shape=jax.ShapeDtypeStruct((slots, width), jnp.float32),
        compiler_params=params(24),
        name="experts",
    )
    keep = serve(own, w_in[0], w_out[0])
    send = serve(other, w_in[0], w_out[0])
    pick, gate = pl.pallas_call(
        gate_body,
        in_specs=[whole] * 4 + [anywhere],
        out_shape=(
            jax.ShapeDtypeStruct((count, slots), jnp.bfloat16),
            jax.ShapeDtypeStruct((count, 128), jnp.float32),
        ),
        compiler_params=params(8),
        name="gate",
    )(outgoing, router_weight.T, expert_row, slot_row, send)
    summed = pl.pallas_call(
        join_body,
        in_specs=[whole] * 2 + [anywhere],
        out_shape=jax.ShapeDtypeStruct((experts, CAP, width), jnp.bfloat16),
        compiler_params=params(8),
        name="join",
    )(keep, lax.ppermute(send, "dp", swap), gate)
    back = exchange(summed)
    block = count // 2
    mixed, update = pl.pallas_call(
        combine_body,
        grid=(count // block,),
        in_specs=[
            pl.BlockSpec((block, width), lambda i: (i, 0)),
            pl.BlockSpec((block, slots), lambda i: (i, 0)),
            pl.BlockSpec((block, 128), lambda i: (i, 0)),
            pl.BlockSpec((experts, CAP, width), lambda i: (0, 0, 0)),
        ],
        out_specs=[
            pl.BlockSpec((block, width), lambda i: (i, 0)),
            pl.BlockSpec((block, width), lambda i: (i, 0)),
        ],
        out_shape=(
            jax.ShapeDtypeStruct((count, width), jnp.bfloat16),
            jax.ShapeDtypeStruct((count, width), jnp.bfloat16),
        ),
        compiler_params=params(12),
        name="combine",
    )(tokens, pick, gate, back)
    return (mixed, update)


def solution(mesh):
    in_specs = (
        P(("dp", "expert"), None),
        P(),
        P(),
        P(("dp", "expert")),
        P(("dp", "expert")),
        P("expert", None, "dp"),
        P("expert", "dp", None),
    )
    out_specs = (P(("dp", "expert"), None), P(("dp", "expert"), None))
    return jax.shard_map(
        per_device, mesh=mesh, in_specs=in_specs, out_specs=out_specs, check_vma=False
    )
```

```python
import jax
import jax.numpy as jnp
from jax import lax
from jax.experimental import pallas as pl
from jax.experimental.pallas import tpu as pltpu
from jax.sharding import PartitionSpec as P

CAP = 4
EPS = 1e-06
MIB = 1024 * 1024
PIECES = 4


def rotation(count):
    return (5 * count) // 8


def slot_of(expert, slot, experts):
    place = (expert + (experts - rotation(experts))) % experts
    return jnp.where(slot >= 0, place * CAP + slot, -1)


def open_body(out_ref):
    out_ref[...] = jnp.zeros(out_ref.shape, out_ref.dtype)


def select_body(opened_ref, tokens_ref, expert_ref, slot_ref, out_ref):
    del opened_ref
    slots, count = out_ref.shape[0], tokens_ref.shape[0]
    flat = slot_of(expert_ref[...], slot_ref[...], slots // CAP)
    rows = lax.broadcasted_iota(jnp.int32, (slots, count), 0)
    select = jnp.where(rows == flat, 1.0, 0.0).astype(jnp.bfloat16)
    out_ref[...] = jnp.dot(select, tokens_ref[...], preferred_element_type=jnp.float32)


def norm_body(values_ref, gain_ref, out_ref):
    values = values_ref[...]
    mean = jnp.mean(values, axis=1, keepdims=True)
    centred = values - mean
    var = jnp.mean(centred * centred, axis=1, keepdims=True)
    normed = centred * lax.rsqrt(var + EPS) * gain_ref[...]
    out_ref[...] = normed.reshape(out_ref.shape).astype(jnp.bfloat16)


def gate_body(normed_ref, router_ref, expert_ref, slot_ref, after_ref, pick_ref, gate_ref):
    del after_ref
    count, slots = pick_ref.shape
    experts = router_ref.shape[0]
    logits = lax.dot_general(
        router_ref[...],
        normed_ref[...].reshape(slots, normed_ref.shape[2]),
        (((1,), (1,)), ((), ())),
        preferred_element_type=jnp.float32,
    )
    top = jnp.max(logits, axis=0, keepdims=True)
    exps = jnp.exp(logits - top)
    probs = exps / jnp.sum(exps, axis=0, keepdims=True)
    place = lax.broadcasted_iota(jnp.int32, probs.shape, 1) // CAP
    owner = (place + rotation(experts)) % experts
    expert = lax.broadcasted_iota(jnp.int32, probs.shape, 0)
    slot_gate = jnp.sum(jnp.where(owner == expert, probs, 0.0), axis=0, keepdims=True)
    flat = slot_of(expert_ref[...], slot_ref[...], experts)
    column = jnp.transpose(jnp.broadcast_to(flat, (128, count)))[:, :1]
    picked = column == lax.broadcasted_iota(jnp.int32, (count, slots), 1)
    pick_ref[...] = jnp.where(picked, 1.0, 0.0).astype(jnp.bfloat16)
    gate = jnp.sum(jnp.where(picked, slot_gate, 0.0), axis=1, keepdims=True)
    gate_ref[...] = jnp.broadcast_to(gate, gate_ref.shape)


def gelu(v):
    inner = 0.7978845608028654 * (v + 0.044715 * (v * v * v))
    return 0.5 * v * (1.0 + jnp.tanh(inner))


def expert_body(own_ref, other_ref, w_in_ref, w_out_ref, keep_ref, send_ref):
    own = own_ref[...].reshape(keep_ref.shape)
    other = other_ref[...].reshape(send_ref.shape)
    rows = jnp.concatenate([own, other], axis=0)
    hidden = gelu(jnp.dot(rows, w_in_ref[...], preferred_element_type=jnp.float32))
    total = jnp.dot(
        hidden.astype(jnp.bfloat16), w_out_ref[...], preferred_element_type=jnp.float32
    )
    keep_ref[...] = total[: own.shape[0]]
    send_ref[...] = total[own.shape[0] :]


def join_body(keep_ref, other_ref, after_ref, out_ref):
    del after_ref
    total = keep_ref[...] + other_ref[...]
    out_ref[...] = total.reshape(out_ref.shape).astype(jnp.bfloat16)


def combine_body(
    tokens_ref, pick_ref, gate_ref, back_ref, mixed_hbm, update_hbm, mixed, update, sems
):
    back = back_ref[...].reshape(pick_ref.shape[1], back_ref.shape[2])
    block = tokens_ref.shape[0] // PIECES
    copies = []
    for piece in range(PIECES):
        rows = pl.ds(piece * block, block)
        value = jnp.dot(pick_ref[rows, :], back, preferred_element_type=jnp.float32)
        update[rows, :] = value.astype(jnp.bfloat16)
        copies.append(
            pltpu.make_async_copy(update.at[rows], update_hbm.at[rows], sems.at[0, piece])
        )
        copies[-1].start()
        value = tokens_ref[rows, :].astype(jnp.float32) + gate_ref[rows, :1] * value
        mixed[rows, :] = value.astype(jnp.bfloat16)
        copies.append(
            pltpu.make_async_copy(mixed.at[rows], mixed_hbm.at[rows], sems.at[1, piece])
        )
        copies[-1].start()
    for copy in copies:
        copy.wait()


def params(limit):
    return pltpu.CompilerParams(vmem_limit_bytes=limit * MIB)


def exchange(blocks):
    count = blocks.shape[0]
    group = [(i + rotation(count)) % count for i in range(count)]
    return lax.all_to_all(
        blocks, "expert", split_axis=0, concat_axis=0, tiled=True, axis_index_groups=[group]
    )


def per_device(tokens, ln_gain, router_weight, routes_expert, route_slot, w_in, w_out):
    count, width = tokens.shape
    experts = router_weight.shape[1]
    slots = experts * CAP
    swap = [(0, 1), (1, 0)]
    anywhere = pl.BlockSpec(memory_space=pl.ANY)
    whole = pl.BlockSpec(memory_space=pltpu.VMEM)
    expert_row = routes_expert.reshape(1, count)
    slot_row = route_slot.reshape(1, count)
    long = pl.CostEstimate(flops=20 * 10**9, bytes_accessed=32 * MIB, transcendentals=0)
    opened = pl.pallas_call(
        open_body,
        out_shape=jax.ShapeDtypeStruct((8, 128), jnp.float32),
        compiler_params=params(8),
        cost_estimate=long,
        name="open",
    )()
    values = pl.pallas_call(
        select_body,
        in_specs=[anywhere] + [whole] * 3,
        out_shape=jax.ShapeDtypeStruct((slots, width), jnp.float32),
        compiler_params=params(8),
        name="select",
    )(opened, tokens, expert_row, slot_row)
    outgoing = pl.pallas_call(
        norm_body,
        out_shape=jax.ShapeDtypeStruct((experts, CAP, width), jnp.bfloat16),
        compiler_params=params(8),
        cost_estimate=long,
        name="norm",
    )(values, ln_gain.reshape(1, width))
    own = exchange(outgoing)
    other = lax.ppermute(own, "dp", swap)
    keep, send = pl.pallas_call(
        expert_body,
        out_shape=(
            jax.ShapeDtypeStruct((slots, width), jnp.float32),
            jax.ShapeDtypeStruct((slots, width), jnp.float32),
        ),
        compiler_params=params(24),
        name="experts",
    )(own, other, w_in[0], w_out[0])
    pick, gate = pl.pallas_call(
        gate_body,
        in_specs=[whole] * 4 + [anywhere],
        out_shape=(
            jax.ShapeDtypeStruct((count, slots), jnp.bfloat16),
            jax.ShapeDtypeStruct((count, 128), jnp.float32),
        ),
        compiler_params=params(8),
        name="gate",
    )(outgoing, router_weight.T, expert_row, slot_row, send)
    summed = pl.pallas_call(
        join_body,
        in_specs=[whole] * 2 + [anywhere],
        out_shape=jax.ShapeDtypeStruct((experts, CAP, width), jnp.bfloat16),
        compiler_params=params(8),
        name="join",
    )(keep, lax.ppermute(send, "dp", swap), gate)
    back = exchange(summed)
    mixed, update = pl.pallas_call(
        combine_body,
        in_specs=[whole] * 4,
        out_specs=[anywhere] * 2,
        scratch_shapes=[
            pltpu.VMEM((count, width), jnp.bfloat16),
            pltpu.VMEM((count, width), jnp.bfloat16),
            pltpu.SemaphoreType.DMA((2, PIECES)),
        ],
        out_shape=(
            jax.ShapeDtypeStruct((count, width), jnp.bfloat16),
            jax.ShapeDtypeStruct((count, width), jnp.bfloat16),
        ),
        compiler_params=params(12),
        name="combine",
    )(tokens, pick, gate, back)
    return (mixed, update)


def solution(mesh):
    in_specs = (
        P(("dp", "expert"), None),
        P(),
        P(),
        P(("dp", "expert")),
        P(("dp", "expert")),
        P("expert", None, "dp"),
        P("expert", "dp", None),
    )
    out_specs = (P(("dp", "expert"), None), P(("dp", "expert"), None))
    return jax.shard_map(
        per_device, mesh=mesh, in_specs=in_specs, out_specs=out_specs, check_vma=False
    )
```

```python
import jax
import jax.numpy as jnp
from jax import lax
from jax.experimental import pallas as pl
from jax.experimental.pallas import tpu as pltpu
from jax.sharding import PartitionSpec as P

CAP = 4
EPS = 1e-06
MIB = 1024 * 1024
PIECES = 4


def rotation(count):
    return (5 * count) // 8


def slot_of(expert, slot, experts):
    place = (expert + (experts - rotation(experts))) % experts
    return jnp.where(slot >= 0, place * CAP + slot, -1)


def open_body(out_ref):
    out_ref[...] = jnp.zeros(out_ref.shape, out_ref.dtype)


def select_body(opened_ref, tokens_ref, expert_ref, slot_ref, out_ref):
    del opened_ref
    slots, count = out_ref.shape[0], tokens_ref.shape[0]
    flat = slot_of(expert_ref[...], slot_ref[...], slots // CAP)
    rows = lax.broadcasted_iota(jnp.int32, (slots, count), 0)
    select = jnp.where(rows == flat, 1.0, 0.0).astype(jnp.bfloat16)
    out_ref[...] = jnp.dot(select, tokens_ref[...], preferred_element_type=jnp.float32)


def norm_body(values_ref, gain_ref, out_ref):
    values = values_ref[...]
    mean = jnp.mean(values, axis=1, keepdims=True)
    centred = values - mean
    var = jnp.mean(centred * centred, axis=1, keepdims=True)
    normed = centred * lax.rsqrt(var + EPS) * gain_ref[...]
    out_ref[...] = normed.reshape(out_ref.shape).astype(jnp.bfloat16)


def gate_body(normed_ref, router_ref, expert_ref, slot_ref, after_ref, pick_ref, gate_ref):
    del after_ref
    count, slots = pick_ref.shape
    experts = router_ref.shape[0]
    logits = lax.dot_general(
        router_ref[...],
        normed_ref[...].reshape(slots, normed_ref.shape[2]),
        (((1,), (1,)), ((), ())),
        preferred_element_type=jnp.float32,
    )
    top = jnp.max(logits, axis=0, keepdims=True)
    exps = jnp.exp(logits - top)
    probs = exps / jnp.sum(exps, axis=0, keepdims=True)
    place = lax.broadcasted_iota(jnp.int32, probs.shape, 1) // CAP
    owner = (place + rotation(experts)) % experts
    expert = lax.broadcasted_iota(jnp.int32, probs.shape, 0)
    slot_gate = jnp.sum(jnp.where(owner == expert, probs, 0.0), axis=0, keepdims=True)
    flat = slot_of(expert_ref[...], slot_ref[...], experts)
    column = jnp.transpose(jnp.broadcast_to(flat, (128, count)))[:, :1]
    picked = column == lax.broadcasted_iota(jnp.int32, (count, slots), 1)
    pick_ref[...] = jnp.where(picked, 1.0, 0.0).astype(jnp.bfloat16)
    gate = jnp.sum(jnp.where(picked, slot_gate, 0.0), axis=1, keepdims=True)
    gate_ref[...] = jnp.broadcast_to(gate, gate_ref.shape)


def gelu(v):
    inner = 0.7978845608028654 * (v + 0.044715 * (v * v * v))
    return 0.5 * v * (1.0 + jnp.tanh(inner))


def expert_body(own_ref, other_ref, w_in_ref, w_out_ref, keep_ref, send_ref):
    own = own_ref[...].reshape(keep_ref.shape)
    other = other_ref[...].reshape(send_ref.shape)
    rows = jnp.concatenate([own, other], axis=0)
    hidden = gelu(jnp.dot(rows, w_in_ref[...], preferred_element_type=jnp.float32))
    total = jnp.dot(
        hidden.astype(jnp.bfloat16), w_out_ref[...], preferred_element_type=jnp.float32
    )
    keep_ref[...] = total[: own.shape[0]]
    send_ref[...] = total[own.shape[0] :]


def join_body(keep_ref, other_ref, after_ref, out_ref):
    del after_ref
    total = keep_ref[...] + other_ref[...]
    out_ref[...] = total.reshape(out_ref.shape).astype(jnp.bfloat16)


def combine_body(
    tokens_ref, pick_ref, gate_ref, back_ref, mixed_hbm, update_hbm, mixed, update, sems
):
    back = back_ref[...].reshape(pick_ref.shape[1], back_ref.shape[2])
    block = tokens_ref.shape[0] // PIECES
    copies = []
    for piece in range(PIECES):
        rows = pl.ds(piece * block, block)
        value = jnp.dot(pick_ref[rows, :], back, preferred_element_type=jnp.float32)
        update[rows, :] = value.astype(jnp.bfloat16)
        copies.append(
            pltpu.make_async_copy(update.at[rows], update_hbm.at[rows], sems.at[0, piece])
        )
        copies[-1].start()
        value = tokens_ref[rows, :].astype(jnp.float32) + gate_ref[rows, :1] * value
        mixed[rows, :] = value.astype(jnp.bfloat16)
        copies.append(
            pltpu.make_async_copy(mixed.at[rows], mixed_hbm.at[rows], sems.at[1, piece])
        )
        copies[-1].start()
    for copy in copies:
        copy.wait()


def params(limit):
    return pltpu.CompilerParams(vmem_limit_bytes=limit * MIB)


def exchange(blocks):
    count = blocks.shape[0]
    order = [(i + rotation(count)) % count for i in range(count)]
    near = [i + count * (i >= count // 2) for i in order]
    far = [i + count * (i < count // 2) for i in order]
    return lax.all_to_all(
        blocks,
        ("dp", "expert"),
        split_axis=0,
        concat_axis=0,
        tiled=True,
        axis_index_groups=[near, far],
    )


def per_device(tokens, ln_gain, router_weight, routes_expert, route_slot, w_in, w_out):
    count, width = tokens.shape
    experts = router_weight.shape[1]
    slots = experts * CAP
    swap = [(0, 1), (1, 0)]
    anywhere = pl.BlockSpec(memory_space=pl.ANY)
    whole = pl.BlockSpec(memory_space=pltpu.VMEM)
    expert_row = routes_expert.reshape(1, count)
    slot_row = route_slot.reshape(1, count)
    long = pl.CostEstimate(flops=20 * 10**9, bytes_accessed=32 * MIB, transcendentals=0)
    opened = pl.pallas_call(
        open_body,
        out_shape=jax.ShapeDtypeStruct((8, 128), jnp.float32),
        compiler_params=params(8),
        cost_estimate=long,
        name="open",
    )()
    values = pl.pallas_call(
        select_body,
        in_specs=[anywhere] + [whole] * 3,
        out_shape=jax.ShapeDtypeStruct((slots, width), jnp.float32),
        compiler_params=params(8),
        name="select",
    )(opened, tokens, expert_row, slot_row)
    outgoing = pl.pallas_call(
        norm_body,
        out_shape=jax.ShapeDtypeStruct((experts, CAP, width), jnp.bfloat16),
        compiler_params=params(8),
        cost_estimate=long,
        name="norm",
    )(values, ln_gain.reshape(1, width))
    own = exchange(outgoing)
    other = lax.ppermute(own, "dp", swap)
    keep, send = pl.pallas_call(
        expert_body,
        out_shape=(
            jax.ShapeDtypeStruct((slots, width), jnp.float32),
            jax.ShapeDtypeStruct((slots, width), jnp.float32),
        ),
        compiler_params=params(24),
        name="experts",
    )(own, other, w_in[0], w_out[0])
    pick, gate = pl.pallas_call(
        gate_body,
        in_specs=[whole] * 4 + [anywhere],
        out_shape=(
            jax.ShapeDtypeStruct((count, slots), jnp.bfloat16),
            jax.ShapeDtypeStruct((count, 128), jnp.float32),
        ),
        compiler_params=params(8),
        name="gate",
    )(outgoing, router_weight.T, expert_row, slot_row, send)
    summed = pl.pallas_call(
        join_body,
        in_specs=[whole] * 2 + [anywhere],
        out_shape=jax.ShapeDtypeStruct((experts, CAP, width), jnp.bfloat16),
        compiler_params=params(8),
        name="join",
    )(keep, lax.ppermute(send, "dp", swap), gate)
    back = exchange(summed)
    mixed, update = pl.pallas_call(
        combine_body,
        in_specs=[whole] * 4,
        out_specs=[anywhere] * 2,
        scratch_shapes=[
            pltpu.VMEM((count, width), jnp.bfloat16),
            pltpu.VMEM((count, width), jnp.bfloat16),
            pltpu.SemaphoreType.DMA((2, PIECES)),
        ],
        out_shape=(
            jax.ShapeDtypeStruct((count, width), jnp.bfloat16),
            jax.ShapeDtypeStruct((count, width), jnp.bfloat16),
        ),
        compiler_params=params(12),
        name="combine",
    )(tokens, pick, gate, back)
    return (mixed, update)


def solution(mesh):
    in_specs = (
        P(("dp", "expert"), None),
        P(),
        P(),
        P(("dp", "expert")),
        P(("dp", "expert")),
        P("expert", None, "dp"),
        P("expert", "dp", None),
    )
    out_specs = (P(("dp", "expert"), None), P(("dp", "expert"), None))
    return jax.shard_map(
        per_device, mesh=mesh, in_specs=in_specs, out_specs=out_specs, check_vma=False
    )
```

```python
import jax
import jax.numpy as jnp
from jax import lax
from jax.experimental import pallas as pl
from jax.experimental.pallas import tpu as pltpu
from jax.sharding import PartitionSpec as P

CAP = 4
EPS = 1e-06
MIB = 1024 * 1024
PIECES = 4


def rotation(count):
    return (5 * count) // 8


def slot_of(expert, slot, experts):
    place = (expert + (experts - rotation(experts))) % experts
    return jnp.where(slot >= 0, place * CAP + slot, -1)


def open_body(out_ref):
    out_ref[...] = jnp.zeros(out_ref.shape, out_ref.dtype)


def select_body(opened_ref, tokens_ref, expert_ref, slot_ref, out_ref):
    del opened_ref
    slots, count = out_ref.shape[0], tokens_ref.shape[0]
    flat = slot_of(expert_ref[...], slot_ref[...], slots // CAP)
    rows = lax.broadcasted_iota(jnp.int32, (slots, count), 0)
    select = jnp.where(rows == flat, 1.0, 0.0).astype(jnp.bfloat16)
    out_ref[...] = jnp.dot(select, tokens_ref[...], preferred_element_type=jnp.float32)


def norm_body(values_ref, gain_ref, out_ref):
    values = values_ref[...]
    mean = jnp.mean(values, axis=1, keepdims=True)
    centred = values - mean
    var = jnp.mean(centred * centred, axis=1, keepdims=True)
    normed = centred * lax.rsqrt(var + EPS) * gain_ref[...]
    out_ref[...] = normed.reshape(out_ref.shape).astype(jnp.bfloat16)


def gate_body(normed_ref, router_ref, expert_ref, slot_ref, after_ref, pick_ref, gate_ref):
    del after_ref
    count, slots = pick_ref.shape
    experts = router_ref.shape[0]
    logits = lax.dot_general(
        router_ref[...],
        normed_ref[...].reshape(slots, normed_ref.shape[2]),
        (((1,), (1,)), ((), ())),
        preferred_element_type=jnp.float32,
    )
    top = jnp.max(logits, axis=0, keepdims=True)
    exps = jnp.exp(logits - top)
    probs = exps / jnp.sum(exps, axis=0, keepdims=True)
    place = lax.broadcasted_iota(jnp.int32, probs.shape, 1) // CAP
    owner = (place + rotation(experts)) % experts
    expert = lax.broadcasted_iota(jnp.int32, probs.shape, 0)
    slot_gate = jnp.sum(jnp.where(owner == expert, probs, 0.0), axis=0, keepdims=True)
    flat = slot_of(expert_ref[...], slot_ref[...], experts)
    column = jnp.transpose(jnp.broadcast_to(flat, (128, count)))[:, :1]
    picked = column == lax.broadcasted_iota(jnp.int32, (count, slots), 1)
    pick_ref[...] = jnp.where(picked, 1.0, 0.0).astype(jnp.bfloat16)
    gate = jnp.sum(jnp.where(picked, slot_gate, 0.0), axis=1, keepdims=True)
    gate_ref[...] = jnp.broadcast_to(gate, gate_ref.shape)


def gelu(v):
    inner = 0.7978845608028654 * (v + 0.044715 * (v * v * v))
    return 0.5 * v * (1.0 + jnp.tanh(inner))


def expert_body(own_ref, other_ref, w_in_ref, w_out_ref, keep_ref, send_ref):
    own = own_ref[...].reshape(keep_ref.shape)
    other = other_ref[...].reshape(send_ref.shape)
    rows = jnp.concatenate([own, other], axis=0)
    hidden = gelu(jnp.dot(rows, w_in_ref[...], preferred_element_type=jnp.float32))
    total = jnp.dot(
        hidden.astype(jnp.bfloat16), w_out_ref[...], preferred_element_type=jnp.float32
    )
    keep_ref[...] = total[: own.shape[0]]
    send_ref[...] = total[own.shape[0] :].astype(send_ref.dtype)


def join_body(keep_ref, other_ref, after_ref, out_ref):
    del after_ref
    total = keep_ref[...] + other_ref[...].astype(jnp.float32)
    out_ref[...] = total.reshape(out_ref.shape).astype(jnp.bfloat16)


def combine_body(
    tokens_ref, pick_ref, gate_ref, back_ref, mixed_hbm, update_hbm, mixed, update, sems
):
    back = back_ref[...].reshape(pick_ref.shape[1], back_ref.shape[2])
    block = tokens_ref.shape[0] // PIECES
    copies = []
    for piece in range(PIECES):
        rows = pl.ds(piece * block, block)
        value = jnp.dot(pick_ref[rows, :], back, preferred_element_type=jnp.float32)
        update[rows, :] = value.astype(jnp.bfloat16)
        copies.append(
            pltpu.make_async_copy(update.at[rows], update_hbm.at[rows], sems.at[0, piece])
        )
        copies[-1].start()
        value = tokens_ref[rows, :].astype(jnp.float32) + gate_ref[rows, :1] * value
        mixed[rows, :] = value.astype(jnp.bfloat16)
        copies.append(
            pltpu.make_async_copy(mixed.at[rows], mixed_hbm.at[rows], sems.at[1, piece])
        )
        copies[-1].start()
    for copy in copies:
        copy.wait()


def params(limit):
    return pltpu.CompilerParams(vmem_limit_bytes=limit * MIB)


def exchange(blocks):
    count = blocks.shape[0]
    order = [(i + rotation(count)) % count for i in range(count)]
    near = [i + count * (i >= count // 2) for i in order]
    far = [i + count * (i < count // 2) for i in order]
    return lax.all_to_all(
        blocks,
        ("dp", "expert"),
        split_axis=0,
        concat_axis=0,
        tiled=True,
        axis_index_groups=[near, far],
    )


def per_device(tokens, ln_gain, router_weight, routes_expert, route_slot, w_in, w_out):
    count, width = tokens.shape
    experts = router_weight.shape[1]
    slots = experts * CAP
    swap = [(0, 1), (1, 0)]
    anywhere = pl.BlockSpec(memory_space=pl.ANY)
    whole = pl.BlockSpec(memory_space=pltpu.VMEM)
    expert_row = routes_expert.reshape(1, count)
    slot_row = route_slot.reshape(1, count)
    long = pl.CostEstimate(flops=20 * 10**9, bytes_accessed=32 * MIB, transcendentals=0)
    opened = pl.pallas_call(
        open_body,
        out_shape=jax.ShapeDtypeStruct((8, 128), jnp.float32),
        compiler_params=params(8),
        cost_estimate=long,
        name="open",
    )()
    values = pl.pallas_call(
        select_body,
        in_specs=[anywhere] + [whole] * 3,
        out_shape=jax.ShapeDtypeStruct((slots, width), jnp.float32),
        compiler_params=params(8),
        name="select",
    )(opened, tokens, expert_row, slot_row)
    outgoing = pl.pallas_call(
        norm_body,
        out_shape=jax.ShapeDtypeStruct((experts, CAP, width), jnp.bfloat16),
        compiler_params=params(8),
        cost_estimate=long,
        name="norm",
    )(values, ln_gain.reshape(1, width))
    own = exchange(outgoing)
    other = lax.ppermute(own, "dp", swap)
    keep, send = pl.pallas_call(
        expert_body,
        out_shape=(
            jax.ShapeDtypeStruct((slots, width), jnp.float32),
            jax.ShapeDtypeStruct((slots, width), jnp.bfloat16),
        ),
        compiler_params=params(24),
        name="experts",
    )(own, other, w_in[0], w_out[0])
    pick, gate = pl.pallas_call(
        gate_body,
        in_specs=[whole] * 4 + [anywhere],
        out_shape=(
            jax.ShapeDtypeStruct((count, slots), jnp.bfloat16),
            jax.ShapeDtypeStruct((count, 128), jnp.float32),
        ),
        compiler_params=params(8),
        name="gate",
    )(outgoing, router_weight.T, expert_row, slot_row, send)
    summed = pl.pallas_call(
        join_body,
        in_specs=[whole] * 2 + [anywhere],
        out_shape=jax.ShapeDtypeStruct((experts, CAP, width), jnp.bfloat16),
        compiler_params=params(8),
        name="join",
    )(keep, lax.ppermute(send, "dp", swap), gate)
    back = exchange(summed)
    mixed, update = pl.pallas_call(
        combine_body,
        in_specs=[whole] * 4,
        out_specs=[anywhere] * 2,
        scratch_shapes=[
            pltpu.VMEM((count, width), jnp.bfloat16),
            pltpu.VMEM((count, width), jnp.bfloat16),
            pltpu.SemaphoreType.DMA((2, PIECES)),
        ],
        out_shape=(
            jax.ShapeDtypeStruct((count, width), jnp.bfloat16),
            jax.ShapeDtypeStruct((count, width), jnp.bfloat16),
        ),
        compiler_params=params(12),
        name="combine",
    )(tokens, pick, gate, back)
    return (mixed, update)


def solution(mesh):
    in_specs = (
        P(("dp", "expert"), None),
        P(),
        P(),
        P(("dp", "expert")),
        P(("dp", "expert")),
        P("expert", None, "dp"),
        P("expert", "dp", None),
    )
    out_specs = (P(("dp", "expert"), None), P(("dp", "expert"), None))
    return jax.shard_map(
        per_device, mesh=mesh, in_specs=in_specs, out_specs=out_specs, check_vma=False
    )
```

```python
import jax
import jax.numpy as jnp
from jax import lax
from jax.experimental import pallas as pl
from jax.experimental.pallas import tpu as pltpu
from jax.sharding import PartitionSpec as P

CAP = 4
EPS = 1e-06
MIB = 1024 * 1024
PIECES = 4


def rotation(count):
    return (5 * count) // 8


def slot_of(expert, slot, experts):
    place = (expert + (experts - rotation(experts))) % experts
    return jnp.where(slot >= 0, place * CAP + slot, -1)


def load_body(tokens_hbm, out_ref, sems):
    block = tokens_hbm.shape[0] // PIECES
    copies = []
    for piece in range(PIECES):
        rows = pl.ds(piece * block, block)
        copies.append(
            pltpu.make_async_copy(tokens_hbm.at[rows], out_ref.at[rows], sems.at[piece])
        )
        copies[-1].start()
    for copy in copies:
        copy.wait()


def select_body(tokens_ref, expert_ref, slot_ref, out_ref):
    slots, count = out_ref.shape[0], tokens_ref.shape[0]
    flat = slot_of(expert_ref[...], slot_ref[...], slots // CAP)
    rows = lax.broadcasted_iota(jnp.int32, (slots, count), 0)
    select = jnp.where(rows == flat, 1.0, 0.0).astype(jnp.bfloat16)
    out_ref[...] = jnp.dot(select, tokens_ref[...], preferred_element_type=jnp.float32)


def norm_body(values_ref, gain_ref, out_ref):
    values = values_ref[...]
    mean = jnp.mean(values, axis=1, keepdims=True)
    centred = values - mean
    var = jnp.mean(centred * centred, axis=1, keepdims=True)
    normed = centred * lax.rsqrt(var + EPS) * gain_ref[...]
    out_ref[...] = normed.reshape(out_ref.shape).astype(jnp.bfloat16)


def gate_body(normed_ref, router_ref, expert_ref, slot_ref, after_ref, pick_ref, gate_ref):
    del after_ref
    count, slots = pick_ref.shape
    experts = router_ref.shape[0]
    logits = lax.dot_general(
        router_ref[...],
        normed_ref[...].reshape(slots, normed_ref.shape[2]),
        (((1,), (1,)), ((), ())),
        preferred_element_type=jnp.float32,
    )
    top = jnp.max(logits, axis=0, keepdims=True)
    exps = jnp.exp(logits - top)
    probs = exps / jnp.sum(exps, axis=0, keepdims=True)
    place = lax.broadcasted_iota(jnp.int32, probs.shape, 1) // CAP
    owner = (place + rotation(experts)) % experts
    expert = lax.broadcasted_iota(jnp.int32, probs.shape, 0)
    slot_gate = jnp.sum(jnp.where(owner == expert, probs, 0.0), axis=0, keepdims=True)
    flat = slot_of(expert_ref[...], slot_ref[...], experts)
    column = jnp.transpose(jnp.broadcast_to(flat, (128, count)))[:, :1]
    picked = column == lax.broadcasted_iota(jnp.int32, (count, slots), 1)
    pick_ref[...] = jnp.where(picked, 1.0, 0.0).astype(jnp.bfloat16)
    gate = jnp.sum(jnp.where(picked, slot_gate, 0.0), axis=1, keepdims=True)
    gate_ref[...] = jnp.broadcast_to(gate, gate_ref.shape)


def gelu(v):
    inner = 0.7978845608028654 * (v + 0.044715 * (v * v * v))
    return 0.5 * v * (1.0 + jnp.tanh(inner))


def expert_body(own_ref, other_ref, w_in_ref, w_out_ref, keep_ref, send_ref):
    own = own_ref[...].reshape(keep_ref.shape)
    other = other_ref[...].reshape(send_ref.shape)
    rows = jnp.concatenate([own, other], axis=0)
    hidden = gelu(jnp.dot(rows, w_in_ref[...], preferred_element_type=jnp.float32))
    total = jnp.dot(
        hidden.astype(jnp.bfloat16), w_out_ref[...], preferred_element_type=jnp.float32
    )
    keep_ref[...] = total[: own.shape[0]]
    send_ref[...] = total[own.shape[0] :].astype(send_ref.dtype)


def join_body(keep_ref, other_ref, after_ref, out_ref):
    del after_ref
    total = keep_ref[...] + other_ref[...].astype(jnp.float32)
    out_ref[...] = total.reshape(out_ref.shape).astype(jnp.bfloat16)


def combine_body(
    tokens_ref, pick_ref, gate_ref, back_ref, mixed_hbm, update_hbm, mixed, update, sems
):
    back = back_ref[...].reshape(pick_ref.shape[1], back_ref.shape[2])
    block = tokens_ref.shape[0] // PIECES
    copies = []
    for piece in range(PIECES):
        rows = pl.ds(piece * block, block)
        value = jnp.dot(pick_ref[rows, :], back, preferred_element_type=jnp.float32)
        update[rows, :] = value.astype(jnp.bfloat16)
        copies.append(
            pltpu.make_async_copy(update.at[rows], update_hbm.at[rows], sems.at[0, piece])
        )
        copies[-1].start()
        value = tokens_ref[rows, :].astype(jnp.float32) + gate_ref[rows, :1] * value
        mixed[rows, :] = value.astype(jnp.bfloat16)
        copies.append(
            pltpu.make_async_copy(mixed.at[rows], mixed_hbm.at[rows], sems.at[1, piece])
        )
        copies[-1].start()
    for copy in copies:
        copy.wait()


def params(limit):
    return pltpu.CompilerParams(vmem_limit_bytes=limit * MIB)


def exchange(blocks):
    count = blocks.shape[0]
    order = [(i + rotation(count)) % count for i in range(count)]
    near = [i + count * (i >= count // 2) for i in order]
    far = [i + count * (i < count // 2) for i in order]
    return lax.all_to_all(
        blocks,
        ("dp", "expert"),
        split_axis=0,
        concat_axis=0,
        tiled=True,
        axis_index_groups=[near, far],
    )


def per_device(tokens, ln_gain, router_weight, routes_expert, route_slot, w_in, w_out):
    count, width = tokens.shape
    experts = router_weight.shape[1]
    slots = experts * CAP
    swap = [(0, 1), (1, 0)]
    anywhere = pl.BlockSpec(memory_space=pl.ANY)
    whole = pl.BlockSpec(memory_space=pltpu.VMEM)
    expert_row = routes_expert.reshape(1, count)
    slot_row = route_slot.reshape(1, count)
    long = pl.CostEstimate(flops=20 * 10**9, bytes_accessed=32 * MIB, transcendentals=0)
    tokens = pl.pallas_call(
        load_body,
        in_specs=[anywhere],
        out_specs=whole,
        out_shape=jax.ShapeDtypeStruct((count, width), jnp.bfloat16),
        scratch_shapes=[pltpu.SemaphoreType.DMA((PIECES,))],
        compiler_params=params(53),
        cost_estimate=long,
        name="load",
    )(tokens)
    values = pl.pallas_call(
        select_body,
        out_shape=jax.ShapeDtypeStruct((slots, width), jnp.float32),
        compiler_params=params(8),
        name="select",
    )(tokens, expert_row, slot_row)
    outgoing = pl.pallas_call(
        norm_body,
        out_shape=jax.ShapeDtypeStruct((experts, CAP, width), jnp.bfloat16),
        compiler_params=params(8),
        cost_estimate=long,
        name="norm",
    )(values, ln_gain.reshape(1, width))
    own = exchange(outgoing)
    other = lax.ppermute(own, "dp", swap)
    keep, send = pl.pallas_call(
        expert_body,
        out_shape=(
            jax.ShapeDtypeStruct((slots, width), jnp.float32),
            jax.ShapeDtypeStruct((slots, width), jnp.bfloat16),
        ),
        compiler_params=params(24),
        name="experts",
    )(own, other, w_in[0], w_out[0])
    pick, gate = pl.pallas_call(
        gate_body,
        in_specs=[whole] * 4 + [anywhere],
        out_shape=(
            jax.ShapeDtypeStruct((count, slots), jnp.bfloat16),
            jax.ShapeDtypeStruct((count, 128), jnp.float32),
        ),
        compiler_params=params(8),
        name="gate",
    )(outgoing, router_weight.T, expert_row, slot_row, send)
    summed = pl.pallas_call(
        join_body,
        in_specs=[whole] * 2 + [anywhere],
        out_shape=jax.ShapeDtypeStruct((experts, CAP, width), jnp.bfloat16),
        compiler_params=params(8),
        name="join",
    )(keep, lax.ppermute(send, "dp", swap), gate)
    back = exchange(summed)
    mixed, update = pl.pallas_call(
        combine_body,
        in_specs=[whole] * 4,
        out_specs=[anywhere] * 2,
        scratch_shapes=[
            pltpu.VMEM((count, width), jnp.bfloat16),
            pltpu.VMEM((count, width), jnp.bfloat16),
            pltpu.SemaphoreType.DMA((2, PIECES)),
        ],
        out_shape=(
            jax.ShapeDtypeStruct((count, width), jnp.bfloat16),
            jax.ShapeDtypeStruct((count, width), jnp.bfloat16),
        ),
        compiler_params=params(12),
        name="combine",
    )(tokens, pick, gate, back)
    return (mixed, update)


def solution(mesh):
    in_specs = (
        P(("dp", "expert"), None),
        P(),
        P(),
        P(("dp", "expert")),
        P(("dp", "expert")),
        P("expert", None, "dp"),
        P("expert", "dp", None),
    )
    out_specs = (P(("dp", "expert"), None), P(("dp", "expert"), None))
    return jax.shard_map(
        per_device, mesh=mesh, in_specs=in_specs, out_specs=out_specs, check_vma=False
    )
```

```python
import jax
import jax.numpy as jnp
from jax import lax
from jax.experimental import pallas as pl
from jax.experimental.pallas import tpu as pltpu
from jax.sharding import PartitionSpec as P

CAP = 4
EPS = 1e-06
MIB = 1024 * 1024
PIECES = 4


def rotation(count):
    return (5 * count) // 8


def slot_of(expert, slot, experts):
    place = (expert + (experts - rotation(experts))) % experts
    return jnp.where(slot >= 0, place * CAP + slot, -1)


def open_body(out_ref):
    out_ref[...] = jnp.zeros(out_ref.shape, out_ref.dtype)


def dispatch_body(opened_ref, tokens_ref, gain_ref, expert_ref, slot_ref, out_ref):
    del opened_ref
    experts, cap, width = out_ref.shape
    slots, count = experts * cap, tokens_ref.shape[0]
    flat = slot_of(expert_ref[...], slot_ref[...], experts)
    rows = lax.broadcasted_iota(jnp.int32, (slots, count), 0)
    select = jnp.where(rows == flat, 1.0, 0.0).astype(jnp.bfloat16)
    values = jnp.dot(select, tokens_ref[...], preferred_element_type=jnp.float32)
    mean = jnp.mean(values, axis=1, keepdims=True)
    centred = values - mean
    var = jnp.mean(centred * centred, axis=1, keepdims=True)
    normed = centred * lax.rsqrt(var + EPS) * gain_ref[...]
    out_ref[...] = normed.reshape(out_ref.shape).astype(jnp.bfloat16)


def gate_body(normed_ref, router_ref, expert_ref, slot_ref, after_ref, pick_ref, gate_ref):
    del after_ref
    count, slots = pick_ref.shape
    experts = router_ref.shape[0]
    logits = lax.dot_general(
        router_ref[...],
        normed_ref[...].reshape(slots, normed_ref.shape[2]),
        (((1,), (1,)), ((), ())),
        preferred_element_type=jnp.float32,
    )
    top = jnp.max(logits, axis=0, keepdims=True)
    exps = jnp.exp(logits - top)
    probs = exps / jnp.sum(exps, axis=0, keepdims=True)
    place = lax.broadcasted_iota(jnp.int32, probs.shape, 1) // CAP
    owner = (place + rotation(experts)) % experts
    expert = lax.broadcasted_iota(jnp.int32, probs.shape, 0)
    slot_gate = jnp.sum(jnp.where(owner == expert, probs, 0.0), axis=0, keepdims=True)
    flat = slot_of(expert_ref[...], slot_ref[...], experts)
    column = jnp.transpose(jnp.broadcast_to(flat, (128, count)))[:, :1]
    picked = column == lax.broadcasted_iota(jnp.int32, (count, slots), 1)
    pick_ref[...] = jnp.where(picked, 1.0, 0.0).astype(jnp.bfloat16)
    gate = jnp.sum(jnp.where(picked, slot_gate, 0.0), axis=1, keepdims=True)
    gate_ref[...] = jnp.broadcast_to(gate, gate_ref.shape)


def gelu(v):
    inner = 0.7978845608028654 * (v + 0.044715 * (v * v * v))
    return 0.5 * v * (1.0 + jnp.tanh(inner))


def expert_body(own_ref, other_ref, w_in_ref, w_out_ref, keep_ref, send_ref):
    own = own_ref[...].reshape(keep_ref.shape)
    other = other_ref[...].reshape(send_ref.shape)
    rows = jnp.concatenate([own, other], axis=0)
    hidden = gelu(jnp.dot(rows, w_in_ref[...], preferred_element_type=jnp.float32))
    total = jnp.dot(
        hidden.astype(jnp.bfloat16), w_out_ref[...], preferred_element_type=jnp.float32
    )
    keep_ref[...] = total[: own.shape[0]]
    send_ref[...] = total[own.shape[0] :].astype(send_ref.dtype)


def join_body(keep_ref, other_ref, after_ref, out_ref):
    del after_ref
    total = keep_ref[...] + other_ref[...].astype(jnp.float32)
    out_ref[...] = total.reshape(out_ref.shape).astype(jnp.bfloat16)


def combine_body(
    tokens_ref, pick_ref, gate_ref, back_ref, mixed_hbm, update_hbm, mixed, update, sems
):
    back = back_ref[...].reshape(pick_ref.shape[1], back_ref.shape[2])
    block = tokens_ref.shape[0] // PIECES
    copies = []
    for piece in range(PIECES):
        rows = pl.ds(piece * block, block)
        value = jnp.dot(pick_ref[rows, :], back, preferred_element_type=jnp.float32)
        update[rows, :] = value.astype(jnp.bfloat16)
        copies.append(
            pltpu.make_async_copy(update.at[rows], update_hbm.at[rows], sems.at[0, piece])
        )
        copies[-1].start()
        value = tokens_ref[rows, :].astype(jnp.float32) + gate_ref[rows, :1] * value
        mixed[rows, :] = value.astype(jnp.bfloat16)
        copies.append(
            pltpu.make_async_copy(mixed.at[rows], mixed_hbm.at[rows], sems.at[1, piece])
        )
        copies[-1].start()
    for copy in copies:
        copy.wait()


def params(limit):
    return pltpu.CompilerParams(vmem_limit_bytes=limit * MIB)


def exchange(blocks):
    count = blocks.shape[0]
    order = [(i + rotation(count)) % count for i in range(count)]
    near = [i + count * (i >= count // 2) for i in order]
    far = [i + count * (i < count // 2) for i in order]
    return lax.all_to_all(
        blocks,
        ("dp", "expert"),
        split_axis=0,
        concat_axis=0,
        tiled=True,
        axis_index_groups=[near, far],
    )


def per_device(tokens, ln_gain, router_weight, routes_expert, route_slot, w_in, w_out):
    count, width = tokens.shape
    experts = router_weight.shape[1]
    slots = experts * CAP
    swap = [(0, 1), (1, 0)]
    anywhere = pl.BlockSpec(memory_space=pl.ANY)
    whole = pl.BlockSpec(memory_space=pltpu.VMEM)
    expert_row = routes_expert.reshape(1, count)
    slot_row = route_slot.reshape(1, count)
    long = pl.CostEstimate(flops=20 * 10**9, bytes_accessed=32 * MIB, transcendentals=0)
    opened = pl.pallas_call(
        open_body,
        out_shape=jax.ShapeDtypeStruct((8, 128), jnp.float32),
        compiler_params=params(8),
        cost_estimate=long,
        name="open",
    )()
    outgoing = pl.pallas_call(
        dispatch_body,
        in_specs=[anywhere] + [whole] * 4,
        out_shape=jax.ShapeDtypeStruct((experts, CAP, width), jnp.bfloat16),
        compiler_params=params(8),
        cost_estimate=long,
        name="dispatch",
    )(opened, tokens, ln_gain.reshape(1, width), expert_row, slot_row)
    own = exchange(outgoing)
    other = lax.ppermute(own, "dp", swap)
    keep, send = pl.pallas_call(
        expert_body,
        out_shape=(
            jax.ShapeDtypeStruct((slots, width), jnp.float32),
            jax.ShapeDtypeStruct((slots, width), jnp.bfloat16),
        ),
        compiler_params=params(24),
        name="experts",
    )(own, other, w_in[0], w_out[0])
    pick, gate = pl.pallas_call(
        gate_body,
        in_specs=[whole] * 4 + [anywhere],
        out_shape=(
            jax.ShapeDtypeStruct((count, slots), jnp.bfloat16),
            jax.ShapeDtypeStruct((count, 128), jnp.float32),
        ),
        compiler_params=params(8),
        name="gate",
    )(outgoing, router_weight.T, expert_row, slot_row, send)
    summed = pl.pallas_call(
        join_body,
        in_specs=[whole] * 2 + [anywhere],
        out_shape=jax.ShapeDtypeStruct((experts, CAP, width), jnp.bfloat16),
        compiler_params=params(8),
        name="join",
    )(keep, lax.ppermute(send, "dp", swap), gate)
    back = exchange(summed)
    mixed, update = pl.pallas_call(
        combine_body,
        in_specs=[whole] * 4,
        out_specs=[anywhere] * 2,
        scratch_shapes=[
            pltpu.VMEM((count, width), jnp.bfloat16),
            pltpu.VMEM((count, width), jnp.bfloat16),
            pltpu.SemaphoreType.DMA((2, PIECES)),
        ],
        out_shape=(
            jax.ShapeDtypeStruct((count, width), jnp.bfloat16),
            jax.ShapeDtypeStruct((count, width), jnp.bfloat16),
        ),
        compiler_params=params(12),
        name="combine",
    )(tokens, pick, gate, back)
    return (mixed, update)


def solution(mesh):
    in_specs = (
        P(("dp", "expert"), None),
        P(),
        P(),
        P(("dp", "expert")),
        P(("dp", "expert")),
        P("expert", None, "dp"),
        P("expert", "dp", None),
    )
    out_specs = (P(("dp", "expert"), None), P(("dp", "expert"), None))
    return jax.shard_map(
        per_device, mesh=mesh, in_specs=in_specs, out_specs=out_specs, check_vma=False
    )
```

```python
import jax
import jax.numpy as jnp
from jax import lax
from jax.experimental import pallas as pl
from jax.experimental.pallas import tpu as pltpu
from jax.sharding import PartitionSpec as P

CAP = 4
EPS = 1e-06
MIB = 1024 * 1024
PIECES = 4


def member(place, count):
    return (place * (count // 2 + 1) + (5 * count) // 8 + 1) % count


def slot_of(expert, slot, experts):
    place = (expert + experts - member(0, experts)) * (experts // 2 + 1) % experts
    return jnp.where(slot >= 0, place * CAP + slot, -1)


def open_body(out_ref):
    out_ref[...] = jnp.zeros(out_ref.shape, out_ref.dtype)


def dispatch_body(opened_ref, tokens_ref, gain_ref, expert_ref, slot_ref, out_ref):
    del opened_ref
    experts, cap, width = out_ref.shape
    slots, count = experts * cap, tokens_ref.shape[0]
    flat = slot_of(expert_ref[...], slot_ref[...], experts)
    rows = lax.broadcasted_iota(jnp.int32, (slots, count), 0)
    select = jnp.where(rows == flat, 1.0, 0.0).astype(jnp.bfloat16)
    values = jnp.dot(select, tokens_ref[...], preferred_element_type=jnp.float32)
    mean = jnp.mean(values, axis=1, keepdims=True)
    centred = values - mean
    var = jnp.mean(centred * centred, axis=1, keepdims=True)
    normed = centred * lax.rsqrt(var + EPS) * gain_ref[...]
    out_ref[...] = normed.reshape(out_ref.shape).astype(jnp.bfloat16)


def gate_body(normed_ref, router_ref, expert_ref, slot_ref, after_ref, pick_ref, gate_ref):
    del after_ref
    count, slots = pick_ref.shape
    experts = router_ref.shape[0]
    logits = lax.dot_general(
        router_ref[...],
        normed_ref[...].reshape(slots, normed_ref.shape[2]),
        (((1,), (1,)), ((), ())),
        preferred_element_type=jnp.float32,
    )
    top = jnp.max(logits, axis=0, keepdims=True)
    exps = jnp.exp(logits - top)
    probs = exps / jnp.sum(exps, axis=0, keepdims=True)
    place = lax.broadcasted_iota(jnp.int32, probs.shape, 1) // CAP
    owner = member(place, experts)
    expert = lax.broadcasted_iota(jnp.int32, probs.shape, 0)
    slot_gate = jnp.sum(jnp.where(owner == expert, probs, 0.0), axis=0, keepdims=True)
    flat = slot_of(expert_ref[...], slot_ref[...], experts)
    column = jnp.transpose(jnp.broadcast_to(flat, (128, count)))[:, :1]
    picked = column == lax.broadcasted_iota(jnp.int32, (count, slots), 1)
    pick_ref[...] = jnp.where(picked, 1.0, 0.0).astype(jnp.bfloat16)
    gate = jnp.sum(jnp.where(picked, slot_gate, 0.0), axis=1, keepdims=True)
    gate_ref[...] = jnp.broadcast_to(gate, gate_ref.shape)


def gelu(v):
    inner = 0.7978845608028654 * (v + 0.044715 * (v * v * v))
    return 0.5 * v * (1.0 + jnp.tanh(inner))


def expert_body(own_ref, other_ref, w_in_ref, w_out_ref, keep_ref, send_ref):
    own = own_ref[...].reshape(keep_ref.shape)
    other = other_ref[...].reshape(send_ref.shape)
    rows = jnp.concatenate([own, other], axis=0)
    hidden = gelu(jnp.dot(rows, w_in_ref[...], preferred_element_type=jnp.float32))
    total = jnp.dot(
        hidden.astype(jnp.bfloat16), w_out_ref[...], preferred_element_type=jnp.float32
    )
    keep_ref[...] = total[: own.shape[0]]
    send_ref[...] = total[own.shape[0] :].astype(send_ref.dtype)


def join_body(keep_ref, other_ref, after_ref, out_ref):
    del after_ref
    total = keep_ref[...] + other_ref[...].astype(jnp.float32)
    out_ref[...] = total.reshape(out_ref.shape).astype(jnp.bfloat16)


def combine_body(
    tokens_ref, pick_ref, gate_ref, back_ref, mixed_hbm, update_hbm, mixed, update, sems
):
    back = back_ref[...].reshape(pick_ref.shape[1], back_ref.shape[2])
    block = tokens_ref.shape[0] // PIECES
    copies = []
    for piece in range(PIECES):
        rows = pl.ds(piece * block, block)
        value = jnp.dot(pick_ref[rows, :], back, preferred_element_type=jnp.float32)
        update[rows, :] = value.astype(jnp.bfloat16)
        copies.append(
            pltpu.make_async_copy(update.at[rows], update_hbm.at[rows], sems.at[0, piece])
        )
        copies[-1].start()
        value = tokens_ref[rows, :].astype(jnp.float32) + gate_ref[rows, :1] * value
        mixed[rows, :] = value.astype(jnp.bfloat16)
        copies.append(
            pltpu.make_async_copy(mixed.at[rows], mixed_hbm.at[rows], sems.at[1, piece])
        )
        copies[-1].start()
    for copy in copies:
        copy.wait()


def params(limit):
    return pltpu.CompilerParams(vmem_limit_bytes=limit * MIB)


def exchange(blocks):
    count = blocks.shape[0]
    order = [member(i, count) for i in range(count)]
    near = [i + count * (i >= count // 2) for i in order]
    far = [i + count * (i < count // 2) for i in order]
    return lax.all_to_all(
        blocks,
        ("dp", "expert"),
        split_axis=0,
        concat_axis=0,
        tiled=True,
        axis_index_groups=[near, far],
    )


def per_device(tokens, ln_gain, router_weight, routes_expert, route_slot, w_in, w_out):
    count, width = tokens.shape
    experts = router_weight.shape[1]
    slots = experts * CAP
    swap = [(0, 1), (1, 0)]
    anywhere = pl.BlockSpec(memory_space=pl.ANY)
    whole = pl.BlockSpec(memory_space=pltpu.VMEM)
    expert_row = routes_expert.reshape(1, count)
    slot_row = route_slot.reshape(1, count)
    long = pl.CostEstimate(flops=20 * 10**9, bytes_accessed=32 * MIB, transcendentals=0)
    opened = pl.pallas_call(
        open_body,
        out_shape=jax.ShapeDtypeStruct((8, 128), jnp.float32),
        compiler_params=params(8),
        cost_estimate=long,
        name="open",
    )()
    outgoing = pl.pallas_call(
        dispatch_body,
        in_specs=[anywhere] + [whole] * 4,
        out_shape=jax.ShapeDtypeStruct((experts, CAP, width), jnp.bfloat16),
        compiler_params=params(8),
        cost_estimate=long,
        name="dispatch",
    )(opened, tokens, ln_gain.reshape(1, width), expert_row, slot_row)
    own = exchange(outgoing)
    other = lax.ppermute(own, "dp", swap)
    keep, send = pl.pallas_call(
        expert_body,
        out_shape=(
            jax.ShapeDtypeStruct((slots, width), jnp.float32),
            jax.ShapeDtypeStruct((slots, width), jnp.bfloat16),
        ),
        compiler_params=params(24),
        name="experts",
    )(own, other, w_in[0], w_out[0])
    pick, gate = pl.pallas_call(
        gate_body,
        in_specs=[whole] * 4 + [anywhere],
        out_shape=(
            jax.ShapeDtypeStruct((count, slots), jnp.bfloat16),
            jax.ShapeDtypeStruct((count, 128), jnp.float32),
        ),
        compiler_params=params(8),
        name="gate",
    )(outgoing, router_weight.T, expert_row, slot_row, send)
    summed = pl.pallas_call(
        join_body,
        in_specs=[whole] * 2 + [anywhere],
        out_shape=jax.ShapeDtypeStruct((experts, CAP, width), jnp.bfloat16),
        compiler_params=params(8),
        name="join",
    )(keep, lax.ppermute(send, "dp", swap), gate)
    back = exchange(summed)
    mixed, update = pl.pallas_call(
        combine_body,
        in_specs=[whole] * 4,
        out_specs=[anywhere] * 2,
        scratch_shapes=[
            pltpu.VMEM((count, width), jnp.bfloat16),
            pltpu.VMEM((count, width), jnp.bfloat16),
            pltpu.SemaphoreType.DMA((2, PIECES)),
        ],
        out_shape=(
            jax.ShapeDtypeStruct((count, width), jnp.bfloat16),
            jax.ShapeDtypeStruct((count, width), jnp.bfloat16),
        ),
        compiler_params=params(12),
        name="combine",
    )(tokens, pick, gate, back)
    return (mixed, update)


def solution(mesh):
    in_specs = (
        P(("dp", "expert"), None),
        P(),
        P(),
        P(("dp", "expert")),
        P(("dp", "expert")),
        P("expert", None, "dp"),
        P("expert", "dp", None),
    )
    out_specs = (P(("dp", "expert"), None), P(("dp", "expert"), None))
    return jax.shard_map(
        per_device, mesh=mesh, in_specs=in_specs, out_specs=out_specs, check_vma=False
    )
```

```python
import jax
import jax.numpy as jnp
from jax import lax
from jax.experimental import pallas as pl
from jax.experimental.pallas import tpu as pltpu
from jax.sharding import PartitionSpec as P

CAP = 4
EPS = 1e-06
MIB = 1024 * 1024
PIECES = 4


def member(place, count):
    return place ^ ((11 * count) // 16)


def slot_of(expert, slot, experts):
    place = member(expert, experts)
    return jnp.where(slot >= 0, place * CAP + slot, -1)


def open_body(out_ref):
    out_ref[...] = jnp.zeros(out_ref.shape, out_ref.dtype)


def dispatch_body(opened_ref, tokens_ref, gain_ref, expert_ref, slot_ref, out_ref):
    del opened_ref
    experts, cap, width = out_ref.shape
    slots, count = experts * cap, tokens_ref.shape[0]
    flat = slot_of(expert_ref[...], slot_ref[...], experts)
    rows = lax.broadcasted_iota(jnp.int32, (slots, count), 0)
    select = jnp.where(rows == flat, 1.0, 0.0).astype(jnp.bfloat16)
    values = jnp.dot(select, tokens_ref[...], preferred_element_type=jnp.float32)
    mean = jnp.mean(values, axis=1, keepdims=True)
    centred = values - mean
    var = jnp.mean(centred * centred, axis=1, keepdims=True)
    normed = centred * lax.rsqrt(var + EPS) * gain_ref[...]
    out_ref[...] = normed.reshape(out_ref.shape).astype(jnp.bfloat16)


def gate_body(normed_ref, router_ref, expert_ref, slot_ref, after_ref, pick_ref, gate_ref):
    del after_ref
    count, slots = pick_ref.shape
    experts = router_ref.shape[0]
    logits = lax.dot_general(
        router_ref[...],
        normed_ref[...].reshape(slots, normed_ref.shape[2]),
        (((1,), (1,)), ((), ())),
        preferred_element_type=jnp.float32,
    )
    top = jnp.max(logits, axis=0, keepdims=True)
    exps = jnp.exp(logits - top)
    probs = exps / jnp.sum(exps, axis=0, keepdims=True)
    place = lax.broadcasted_iota(jnp.int32, probs.shape, 1) // CAP
    owner = member(place, experts)
    expert = lax.broadcasted_iota(jnp.int32, probs.shape, 0)
    slot_gate = jnp.sum(jnp.where(owner == expert, probs, 0.0), axis=0, keepdims=True)
    flat = slot_of(expert_ref[...], slot_ref[...], experts)
    column = jnp.transpose(jnp.broadcast_to(flat, (128, count)))[:, :1]
    picked = column == lax.broadcasted_iota(jnp.int32, (count, slots), 1)
    pick_ref[...] = jnp.where(picked, 1.0, 0.0).astype(jnp.bfloat16)
    gate = jnp.sum(jnp.where(picked, slot_gate, 0.0), axis=1, keepdims=True)
    gate_ref[...] = jnp.broadcast_to(gate, gate_ref.shape)


def gelu(v):
    inner = 0.7978845608028654 * (v + 0.044715 * (v * v * v))
    return 0.5 * v * (1.0 + jnp.tanh(inner))


def expert_body(own_ref, other_ref, w_in_ref, w_out_ref, keep_ref, send_ref):
    own = own_ref[...].reshape(keep_ref.shape)
    other = other_ref[...].reshape(send_ref.shape)
    rows = jnp.concatenate([own, other], axis=0)
    hidden = gelu(jnp.dot(rows, w_in_ref[...], preferred_element_type=jnp.float32))
    total = jnp.dot(
        hidden.astype(jnp.bfloat16), w_out_ref[...], preferred_element_type=jnp.float32
    )
    keep_ref[...] = total[: own.shape[0]]
    send_ref[...] = total[own.shape[0] :].astype(send_ref.dtype)


def join_body(keep_ref, other_ref, after_ref, out_ref):
    del after_ref
    total = keep_ref[...] + other_ref[...].astype(jnp.float32)
    out_ref[...] = total.reshape(out_ref.shape).astype(jnp.bfloat16)


def combine_body(
    tokens_ref, pick_ref, gate_ref, back_ref, mixed_hbm, update_hbm, mixed, update, sems
):
    back = back_ref[...].reshape(pick_ref.shape[1], back_ref.shape[2])
    block = tokens_ref.shape[0] // PIECES
    copies = []
    for piece in range(PIECES):
        rows = pl.ds(piece * block, block)
        value = jnp.dot(pick_ref[rows, :], back, preferred_element_type=jnp.float32)
        update[rows, :] = value.astype(jnp.bfloat16)
        copies.append(
            pltpu.make_async_copy(update.at[rows], update_hbm.at[rows], sems.at[0, piece])
        )
        copies[-1].start()
        value = tokens_ref[rows, :].astype(jnp.float32) + gate_ref[rows, :1] * value
        mixed[rows, :] = value.astype(jnp.bfloat16)
        copies.append(
            pltpu.make_async_copy(mixed.at[rows], mixed_hbm.at[rows], sems.at[1, piece])
        )
        copies[-1].start()
    for copy in copies:
        copy.wait()


def params(limit):
    return pltpu.CompilerParams(vmem_limit_bytes=limit * MIB)


def exchange(blocks):
    count = blocks.shape[0]
    order = [member(i, count) for i in range(count)]
    near = [i + count * (i >= count // 2) for i in order]
    far = [i + count * (i < count // 2) for i in order]
    return lax.all_to_all(
        blocks,
        ("dp", "expert"),
        split_axis=0,
        concat_axis=0,
        tiled=True,
        axis_index_groups=[near, far],
    )


def per_device(tokens, ln_gain, router_weight, routes_expert, route_slot, w_in, w_out):
    count, width = tokens.shape
    experts = router_weight.shape[1]
    slots = experts * CAP
    swap = [(0, 1), (1, 0)]
    anywhere = pl.BlockSpec(memory_space=pl.ANY)
    whole = pl.BlockSpec(memory_space=pltpu.VMEM)
    expert_row = routes_expert.reshape(1, count)
    slot_row = route_slot.reshape(1, count)
    long = pl.CostEstimate(flops=20 * 10**9, bytes_accessed=32 * MIB, transcendentals=0)
    opened = pl.pallas_call(
        open_body,
        out_shape=jax.ShapeDtypeStruct((8, 128), jnp.float32),
        compiler_params=params(8),
        cost_estimate=long,
        name="open",
    )()
    outgoing = pl.pallas_call(
        dispatch_body,
        in_specs=[anywhere] + [whole] * 4,
        out_shape=jax.ShapeDtypeStruct((experts, CAP, width), jnp.bfloat16),
        compiler_params=params(8),
        cost_estimate=long,
        name="dispatch",
    )(opened, tokens, ln_gain.reshape(1, width), expert_row, slot_row)
    own = exchange(outgoing)
    other = lax.ppermute(own, "dp", swap)
    keep, send = pl.pallas_call(
        expert_body,
        out_shape=(
            jax.ShapeDtypeStruct((slots, width), jnp.float32),
            jax.ShapeDtypeStruct((slots, width), jnp.bfloat16),
        ),
        compiler_params=params(24),
        name="experts",
    )(own, other, w_in[0], w_out[0])
    pick, gate = pl.pallas_call(
        gate_body,
        in_specs=[whole] * 4 + [anywhere],
        out_shape=(
            jax.ShapeDtypeStruct((count, slots), jnp.bfloat16),
            jax.ShapeDtypeStruct((count, 128), jnp.float32),
        ),
        compiler_params=params(8),
        name="gate",
    )(outgoing, router_weight.T, expert_row, slot_row, send)
    summed = pl.pallas_call(
        join_body,
        in_specs=[whole] * 2 + [anywhere],
        out_shape=jax.ShapeDtypeStruct((experts, CAP, width), jnp.bfloat16),
        compiler_params=params(8),
        name="join",
    )(keep, lax.ppermute(send, "dp", swap), gate)
    back = exchange(summed)
    mixed, update = pl.pallas_call(
        combine_body,
        in_specs=[whole] * 4,
        out_specs=[anywhere] * 2,
        scratch_shapes=[
            pltpu.VMEM((count, width), jnp.bfloat16),
            pltpu.VMEM((count, width), jnp.bfloat16),
            pltpu.SemaphoreType.DMA((2, PIECES)),
        ],
        out_shape=(
            jax.ShapeDtypeStruct((count, width), jnp.bfloat16),
            jax.ShapeDtypeStruct((count, width), jnp.bfloat16),
        ),
        compiler_params=params(12),
        name="combine",
    )(tokens, pick, gate, back)
    return (mixed, update)


def solution(mesh):
    in_specs = (
        P(("dp", "expert"), None),
        P(),
        P(),
        P(("dp", "expert")),
        P(("dp", "expert")),
        P("expert", None, "dp"),
        P("expert", "dp", None),
    )
    out_specs = (P(("dp", "expert"), None), P(("dp", "expert"), None))
    return jax.shard_map(
        per_device, mesh=mesh, in_specs=in_specs, out_specs=out_specs, check_vma=False
    )
```
